32 devices in a mesh: seq: 4 (over y, x), tp: 4 (over z), grp: 2 (over core).
Axes of the slice: x: 2, y: 2, z: 4, core: 2. Of those that a mesh axis runs over, the one named last changes fastest.
Arguments:
- query: bfloat16 [16, 64, 8192], P('grp', None, 'tp'), parts along dimension 0, may hold values from -15 to 15
- cache: bfloat16 [16, 4096, 8, 256], P('grp', 'tp', 'seq'), parts along dimension 0, may hold values from -6 to 6
- head_of_slot: int32 [16], P('grp'), parts along dimension 0, may hold values from 0 to 7, each once
- lengths: int32 [16], P('grp'), parts along dimension 0, may hold values from 2048 to 4096
- out_weight: bfloat16 [8192, 8192], P('tp', 'seq'), may hold values from -0.0625 to 0.0625
Outputs:
- projected: bfloat16 [16, 64, 8192], P(('grp', 'tp'), None, 'seq'), parts along dimension 0
The draws below stay inside these ranges and needn't reach their ends.
There are 2 independent parts, one for each index of `grp`. The reference program is written for one: setup_inputs(seed, part) draws one part's arguments, and reference() takes and returns one part's arrays. A program takes and returns all parts, laid end to end along the dimension named above; an argument that names none is the same for every part. Nothing has to cross between parts.
Inputs may be any that keep to these rules, and one draw needn't show every extreme that they name: head_of_slot names every KV head exactly once.
All inputs are finite; a program needn't handle non-finite values.
Results may differ from the reference program's by a relative error of at most 0.01.
Values may be sent and summed in bfloat16 or wider, within the bound.
A program may use at most 128 MiB of HBM per device.

```python
import math
import jax
import jax.numpy as jnp
from jax import lax

D = 8192
HQ = 64
KVH = 8
HD = 128
B = 8
QT = 64
L = 4096


def draw_query(key, part):
    own_key = jax.random.fold_in(key, 11)
    values = jnp.clip(3.0 * jax.random.normal(own_key, (B, QT, HQ * HD), jnp.float32), -15.0, 15.0)
    return values.astype(jnp.bfloat16)


def draw_cache(key, part):
    own_key = jax.random.fold_in(key, 23)
    values = jnp.clip(jax.random.normal(own_key, (B, L, KVH, 2 * HD), jnp.float32), -6.0, 6.0)
    return values.astype(jnp.bfloat16)


def with_ends(values, key, smallest, top_value):
    shape = values.shape
    spot = [jax.random.randint(jax.random.fold_in(key, axis), (), 0, shape[axis]) for axis in range(len(shape))]
    values = values.at[tuple(spot)].set(smallest)
    longest = shape.index(max(shape))
    spot[longest] = (spot[longest] + 1) % shape[longest]
    return values.at[tuple(spot)].set(top_value)


def shard_levels(stream_key, extent, shards, smallest, top_value):
    factor_of = 1.0
    for position, parts in shards:
        heights = jax.random.uniform(jax.random.fold_in(jax.random.fold_in(stream_key, 6), position), (parts,), jnp.float32, smallest / len(shards), top_value / len(shards))
        factor_of = factor_of * jnp.repeat(jnp.exp(heights), extent[position] // parts).reshape((-1,) + (1,) * (len(extent) - 1 - position))
    return factor_of


def noise(key, shape, spread, bound, cuts=(), kind=jnp.bfloat16):
    loudness = shard_levels(key, shape, cuts, -0.22, 0.18) if cuts else 1.0
    drawn = jax.random.normal(key, shape, jnp.float32) * spread * loudness
    return jnp.minimum(jnp.maximum(drawn, -bound), bound).astype(kind)


def setup_inputs(seed: int = 0, part: int = 0) -> dict:
    arg_keys = jax.random.split(jax.random.key(seed), 6)
    own_keys = jax.random.split(jax.random.fold_in(arg_keys[5], part), 6)
    query = draw_query(jax.random.fold_in(jax.random.fold_in(arg_keys[5], part), 71), part)
    cache = draw_cache(jax.random.fold_in(jax.random.fold_in(arg_keys[5], part), 71), part)
    head_of_slot = jax.random.permutation(own_keys[2], KVH).astype(jnp.int32)
    lengths = with_ends(jax.random.randint(own_keys[3], (B,), L // 2, L + 1), jax.random.fold_in(own_keys[3], 1), L // 2, L).astype(jnp.int32)
    out_weight = noise(arg_keys[4], (HQ * HD, D), (HQ * HD) ** -0.5, 0.0625, ((0, 4), (1, 4)))
    return dict(query=query, cache=cache, head_of_slot=head_of_slot, lengths=lengths, out_weight=out_weight)


MASKED_SCORE = -1e+30

def reference(query, cache, head_of_slot, lengths, out_weight):
    group_size = HQ // KVH
    scaling = 1.0 / math.sqrt(HD)
    slot_ids = jnp.arange(KVH, dtype=jnp.int32)
    slot_of_head = lax.optimization_barrier(jnp.sum(jnp.where(head_of_slot[None, :] == slot_ids[:, None], slot_ids[None, :], 0), axis=1)).astype(jnp.int32)
    positions = jnp.arange(L, dtype=jnp.int32)
    row_token = jnp.arange(QT * group_size, dtype=jnp.int32) // group_size

    def attend_pair(pair_index):
        seq_index = pair_index // KVH
        kv_head = pair_index % KVH
        entries = lax.dynamic_index_in_dim(cache, seq_index, 0, False)
        entries = lax.dynamic_index_in_dim(entries, slot_of_head[kv_head], 1, False)
        queries = lax.dynamic_index_in_dim(query, seq_index, 0, False)
        queries = lax.dynamic_slice_in_dim(queries, kv_head * group_size * HD, group_size * HD, 1)
        queries = queries.reshape(QT * group_size, HD)
        scores = jnp.dot(queries, entries[:, :HD].T, preferred_element_type=jnp.float32) * scaling
        limits = lengths[seq_index] - QT + row_token
        visible = positions[None, :] <= limits[:, None]
        scores = jnp.where(visible, scores, MASKED_SCORE)
        maxima = lax.optimization_barrier(jnp.max(scores, axis=1))
        weights = jnp.where(visible, jnp.exp(scores - maxima[:, None]), 0.0)
        totals = lax.optimization_barrier(jnp.sum(weights, axis=1))
        blended = jnp.dot(weights.astype(jnp.bfloat16), entries[:, HD:], preferred_element_type=jnp.float32)
        return (blended / totals[:, None]).astype(jnp.bfloat16).reshape(QT, group_size * HD)
    attended = lax.map(attend_pair, jnp.arange(B * KVH, dtype=jnp.int32))
    attended = attended.reshape(B, KVH, QT, group_size * HD).transpose(0, 2, 1, 3).reshape(B * QT, HQ * HD)
    projected = jnp.dot(attended, out_weight, preferred_element_type=jnp.float32)
    return projected.astype(jnp.bfloat16).reshape(B, QT, D)
```

```python
import functools
import math

import jax
import jax.numpy as jnp
from jax import lax
from jax.experimental import pallas as pl
from jax.experimental.pallas import tpu as pltpu
from jax.sharding import PartitionSpec as P

HQ = 64
KVH = 8
CHUNKS = 2
MASKED_SCORE = -1e30
FLOOR = -1e29


def send(block, axis, step):
    n = lax.axis_size(axis)
    return lax.ppermute(block, axis, [(i, i ^ step) for i in range(n)])


def exchange(pick, axis):
    return [pick(0)] + [send(pick(k), axis, k) for k in range(1, lax.axis_size(axis))]


def slot_table(head_of_slot):
    slot_total = head_of_slot.shape[0]
    slot_ids = jnp.arange(slot_total, dtype=jnp.int32)
    return jnp.sum(
        jnp.where(head_of_slot[None, :] == slot_ids[:, None], slot_ids[None, :], 0), axis=1
    )


def attend(q, kv, lengths, rank_seq, first_pos, part, group, bq, tp):
    n_src, ns, nsq, G, T, hd = q.shape
    B, Lb = kv.shape[1], kv.shape[2]
    per_tp = B // tp
    nb = n_src * nsq
    rows = G * T
    block = math.gcd(Lb, 256)
    scale = math.log2(math.e) / math.sqrt(hd)

    def chunk_seq(p, n, meta):
        return (meta[0] ^ p) * nsq + n

    def whole_seq(p, n, meta):
        b = chunk_seq(p, n, meta)
        return (b // bq) * per_tp + part * bq + b % bq

    def kernel(meta, len_ref, q_ref, kv_ref, o_ref, lse_ref, scores):
        b = whole_seq(pl.program_id(1), pl.program_id(2), meta)
        visible_end = len_ref[b] - meta[1]
        turns = jnp.clip((visible_end + block - 1) // block, 0, Lb // block)
        queries = q_ref[...].reshape(rows, hd)
        token = lax.broadcasted_iota(jnp.int32, (1, rows), 1) % T
        limits = visible_end - T + token

        def score(k, top):
            at = pl.multiple_of(k * block, block)
            s = lax.dot_general(
                kv_ref[0, 0, pl.ds(at, block), :hd],
                queries,
                (((1,), (1,)), ((), ())),
                preferred_element_type=jnp.float32,
            )
            pos = at + lax.broadcasted_iota(jnp.int32, (block, 1), 0)
            s = jnp.where(pos <= limits, s * scale, MASKED_SCORE)
            scores[pl.ds(at, block), :] = s
            return jnp.maximum(top, jnp.max(s, axis=0, keepdims=True))

        top = lax.fori_loop(0, turns, score, jnp.full((1, rows), FLOOR, jnp.float32))

        def blend(k, carried):
            total, out = carried
            at = pl.multiple_of(k * block, block)
            w = jnp.exp2(scores[pl.ds(at, block), :] - top)
            total = total + jnp.sum(w, axis=0, keepdims=True)
            out = out + lax.dot_general(
                kv_ref[0, 0, pl.ds(at, block), hd:],
                w.astype(jnp.bfloat16),
                (((0,), (0,)), ((), ())),
                preferred_element_type=jnp.float32,
            )
            return total, out

        total, out = lax.fori_loop(
            0,
            turns,
            blend,
            (jnp.zeros((1, rows), jnp.float32), jnp.zeros((hd, rows), jnp.float32)),
        )
        total = jnp.maximum(total, 1e-30)
        o_ref[0, 0] = (out / total).astype(jnp.bfloat16)
        lse_ref[0, 0] = top + jnp.log2(total)

    meta = jnp.stack([rank_seq, first_pos]).astype(jnp.int32)
    return pl.pallas_call(
        kernel,
        out_shape=(
            jax.ShapeDtypeStruct((nb, ns, hd, rows), jnp.bfloat16),
            jax.ShapeDtypeStruct((nb, ns, 1, rows), jnp.float32),
        ),
        grid_spec=pltpu.PrefetchScalarGridSpec(
            num_scalar_prefetch=2,
            grid=(ns, n_src, nsq),
            in_specs=[
                pl.BlockSpec(
                    (1, 1, 1, G, T, hd), lambda s, p, n, meta, lens: (p, s, n, 0, 0, 0)
                ),
                pl.BlockSpec(
                    (1, 1, Lb, 2 * hd),
                    lambda s, p, n, meta, lens: (s, whole_seq(p, n, meta), 0, 0),
                ),
            ],
            out_specs=[
                pl.BlockSpec(
                    (1, 1, hd, rows), lambda s, p, n, meta, lens: (chunk_seq(p, n, meta), s, 0, 0)
                ),
                pl.BlockSpec(
                    (1, 1, 1, rows), lambda s, p, n, meta, lens: (chunk_seq(p, n, meta), s, 0, 0)
                ),
            ],
            scratch_shapes=[pltpu.VMEM((Lb, rows), jnp.float32)],
        ),
        compiler_params=pltpu.CompilerParams(
            dimension_semantics=("arbitrary", "arbitrary", "arbitrary")
        ),
        cost_estimate=pl.CostEstimate(
            flops=nb * ns * rows * Lb * hd * 6,
            bytes_accessed=nb * ns * (rows * hd * 4 + Lb * hd * 4),
            transcendentals=nb * ns * rows * Lb,
        ),
    )(meta, lengths, q, kv)


def local(query, cache, head_of_slot, lengths, out_weight):
    G = HQ // KVH
    n_seq, n_tp = lax.axis_size("seq"), lax.axis_size("tp")
    me_s, me_t = lax.axis_index("seq"), lax.axis_index("tp")
    slot_of_head = slot_table(head_of_slot)
    B, T, width = query.shape
    Lb, ns, hd2 = cache.shape[1:]
    hd = hd2 // 2
    hl = KVH // n_tp
    per_tp = B // n_tp
    nc = math.gcd(CHUNKS, per_tp)
    bq = per_tp // nc
    nsq = n_tp * bq // n_seq
    sub = T // n_seq

    def at(array, index):
        return lax.dynamic_index_in_dim(array, index, 0, False)

    qh = query.reshape(n_tp, nc, bq, T, hl * G, hd).transpose(1, 0, 2, 4, 3, 5)
    qh = qh.reshape(nc, n_seq, nsq, hl, G, T, hd)
    kv = cache.transpose(2, 0, 1, 3)

    gathered = []
    for c in range(nc):
        mine = at(qh[c], me_s).transpose(1, 0, 2, 3, 4)
        gathered.append(exchange(lambda k: mine, "tp"))

    queries = []
    for c in range(nc):
        pool = jnp.stack(gathered[c])

        def for_column(k):
            blocks = []
            for j in range(ns):
                head = head_of_slot[(me_s ^ k) * ns + j]
                blocks.append(
                    lax.dynamic_slice(
                        pool,
                        (me_t ^ (head // hl), head % hl, 0, 0, 0, 0),
                        (1, 1, nsq, G, T, hd),
                    )[0, 0]
                )
            return jnp.stack(blocks)

        queries.append(jnp.stack(exchange(for_column, "seq")))

    outputs = []
    for c in range(nc):
        o, lse = attend(queries[c], kv, lengths, me_s, me_t * Lb, c, G, bq, n_tp)
        o = o.reshape(n_tp, bq, ns, hd, G * T)
        lse = lse.reshape(n_tp, bq, ns, 1, G * T)
        os_ = exchange(lambda k: at(o, me_t ^ k), "tp")
        ls_ = exchange(lambda k: at(lse, me_t ^ k), "tp")
        top = functools.reduce(jnp.maximum, ls_)
        ws = [jnp.exp2(l - top) for l in ls_]
        total = sum(ws)
        att = sum(w * x.astype(jnp.float32) for w, x in zip(ws, os_)) / total
        att = att.astype(jnp.bfloat16).reshape(bq, ns, hd, G, n_seq, sub)
        att = att.transpose(4, 1, 0, 5, 3, 2).reshape(n_seq, ns, bq, sub, G * hd)
        slots = jnp.stack(exchange(lambda k: at(att, me_s ^ k), "seq"))

        def for_plane(k):
            parts = []
            for j in range(hl):
                slot = slot_of_head[(me_t ^ k) * hl + j]
                parts.append(
                    lax.dynamic_slice(
                        slots,
                        (me_s ^ (slot // ns), slot % ns, 0, 0, 0),
                        (1, 1, bq, sub, G * hd),
                    )[0, 0]
                )
            return jnp.concatenate(parts, axis=-1)

        rows = jnp.stack(exchange(for_plane, "tp"))
        full = exchange(lambda k: rows, "seq")
        full = jnp.stack(full, axis=1)
        partial = jnp.dot(
            full.reshape(n_tp, n_seq * bq * sub, width),
            out_weight,
            preferred_element_type=jnp.float32,
        )
        received = [partial[0]] + [
            send(partial[k].astype(jnp.bfloat16), "tp", k).astype(jnp.float32)
            for k in range(1, n_tp)
        ]
        summed = sum(received).astype(jnp.bfloat16).reshape(n_seq, bq, sub, -1)
        ordered = jnp.stack([at(summed, me_s ^ p) for p in range(n_seq)], axis=1)
        outputs.append(ordered.reshape(bq, T, -1))
    return jnp.concatenate(outputs, axis=0)


def solution(mesh):
    in_specs = (
        P("grp", None, "tp"),
        P("grp", "tp", "seq", None),
        P("grp"),
        P("grp"),
        P("tp", "seq"),
    )
    out_specs = P(("grp", "tp"), None, "seq")
    return jax.shard_map(local, mesh=mesh, in_specs=in_specs, out_specs=out_specs, check_vma=False)
```

```python
import functools
import math

import jax
import jax.numpy as jnp
from jax import lax
from jax.experimental import pallas as pl
from jax.experimental.pallas import tpu as pltpu
from jax.sharding import PartitionSpec as P

HQ = 64
KVH = 8
CHUNKS = 2
MASKED_SCORE = -1e30
FLOOR = -1e29
MESH = pl.DeviceIdType.MESH


def slot_table(head_of_slot):
    slot_total = head_of_slot.shape[0]
    slot_ids = jnp.arange(slot_total, dtype=jnp.int32)
    return jnp.sum(
        jnp.where(head_of_slot[None, :] == slot_ids[:, None], slot_ids[None, :], 0), axis=1
    )


def greet(axes):
    barrier = pltpu.get_barrier_semaphore()
    total = 0
    for axis in axes:
        n = lax.axis_size(axis)
        me = lax.axis_index(axis)
        for k in range(1, n):
            pl.semaphore_signal(
                barrier, inc=1, device_id={axis: lax.rem(me + k, n)}, device_id_type=MESH
            )
            total += 1
    pl.semaphore_wait(barrier, total)


def remote(src, dst, send_sem, recv_sem, axis, k):
    n = lax.axis_size(axis)
    target = lax.rem(lax.axis_index(axis) + k, n)
    return pltpu.make_async_remote_copy(
        src_ref=src,
        dst_ref=dst,
        send_sem=send_sem,
        recv_sem=recv_sem,
        device_id={axis: target},
        device_id_type=MESH,
    )


def back(axis, index):
    n = lax.axis_size(axis)
    return lax.rem(lax.axis_index(axis) + n - index, n)


def gather_attend_kernel(
    dims, hos, lens, q_ref, kv_ref, att_ref,
    zq, xs, xr, osend, orecv, lsend, lrecv, scores,
    zq_s, zq_r, xq_s, xq_r, o_s, o_r, l_s, l_r, own_sem,
):
    nc, bq, nsq, hl, ns, per_tp, Lb, hd, G, T = dims
    n_tp, n_seq = lax.axis_size("tp"), lax.axis_size("seq")
    me_t, me_s = lax.axis_index("tp"), lax.axis_index("seq")
    rows = G * T
    block = math.gcd(Lb, 256)
    scale = math.log2(math.e) / math.sqrt(hd)
    greet(("tp", "seq"))

    zsends = [
        [remote(q_ref.at[c], zq[c].at[k], zq_s.at[c, k], zq_r.at[c, k], "tp", k) for k in range(1, n_tp)]
        for c in range(nc)
    ]
    owns = [pltpu.make_async_copy(q_ref.at[c], zq[c].at[0], own_sem.at[c]) for c in range(nc)]
    for c in range(nc):
        for copy in zsends[c]:
            copy.start()
        owns[c].start()

    xsends = [
        [remote(xs.at[c, k], xr.at[c, k], xq_s.at[c, k], xq_r.at[c, k], "seq", k) for k in range(1, n_seq)]
        for c in range(nc)
    ]

    def spread(c):
        owns[c].wait()
        for copy in zsends[c]:
            copy.wait_recv()
        for k in list(range(1, n_seq)) + [0]:
            target = xr if k == 0 else xs
            column = lax.rem(me_s + k, n_seq)
            for j in range(ns):
                head = hos[column * ns + j]
                target[c, k, j] = zq[c][back("tp", head // hl), head % hl]
            if k:
                xsends[c][k - 1].start()

    osends = [
        [remote(osend.at[c, k], orecv.at[c, k], o_s.at[c, k], o_r.at[c, k], "tp", k) for k in range(1, n_tp)]
        for c in range(nc)
    ]
    lsends = [
        [remote(lsend.at[c, k], lrecv.at[c, k], l_s.at[c, k], l_r.at[c, k], "tp", k) for k in range(1, n_tp)]
        for c in range(nc)
    ]

    def attend_pair(c, k, pair):
        x, slot = pair // ns, pair % ns
        plane = lax.rem(me_t + k, n_tp)
        local_seq = plane * bq + x
        whole_seq = plane * per_tp + c * bq + x
        source = back("seq", local_seq // nsq)
        queries = xr[c, source, slot, local_seq % nsq].reshape(rows, hd)
        visible_end = lens[whole_seq] - me_t * Lb
        limits = visible_end - T + lax.broadcasted_iota(jnp.int32, (1, rows), 1) % T
        top = jnp.full((1, rows), FLOOR, jnp.float32)
        for i in range(Lb // block):
            s = lax.dot_general(
                kv_ref[slot, whole_seq, i * block : (i + 1) * block, :hd],
                queries,
                (((1,), (1,)), ((), ())),
                preferred_element_type=jnp.float32,
            )
            pos = i * block + lax.broadcasted_iota(jnp.int32, (block, 1), 0)
            s = jnp.where(pos <= limits, s * scale, MASKED_SCORE)
            scores[i * block : (i + 1) * block, :] = s
            top = jnp.maximum(top, jnp.max(s, axis=0, keepdims=True))
        total = jnp.zeros((1, rows), jnp.float32)
        out = jnp.zeros((hd, rows), jnp.float32)
        for i in range(Lb // block):
            w = jnp.exp2(scores[i * block : (i + 1) * block, :] - top)
            total = total + jnp.sum(w, axis=0, keepdims=True)
            out = out + lax.dot_general(
                kv_ref[slot, whole_seq, i * block : (i + 1) * block, hd:],
                w.astype(jnp.bfloat16),
                (((0,), (0,)), ((), ())),
                preferred_element_type=jnp.float32,
            )
        total = jnp.maximum(total, 1e-30)
        o_to, l_to = (orecv, lrecv) if k == 0 else (osend, lsend)
        o_to[c, k, x, slot] = (out / total).astype(jnp.bfloat16)
        l_to[c, k, x, slot] = top + jnp.log2(total)

    def attend(c):
        for copy in xsends[c]:
            copy.wait_recv()
        order = sorted(range(1, n_tp), key=lambda k: abs(k - n_tp / 2)) + [0]
        for k in order:
            lax.fori_loop(0, bq * ns, lambda pair, _: (attend_pair(c, k, pair), 0)[1], 0)
            if k:
                osends[c][k - 1].start()
                lsends[c][k - 1].start()

    def merge(c):
        for k in range(n_tp - 1):
            osends[c][k].wait_recv()
            lsends[c][k].wait_recv()

        def one(pair, _):
            x, slot = pair // ns, pair % ns
            ls = [lrecv[c, k, x, slot] for k in range(n_tp)]
            top = functools.reduce(jnp.maximum, ls)
            ws = [jnp.exp2(l - top) for l in ls]
            inverse = 1.0 / sum(ws)
            out = jnp.zeros((hd, rows), jnp.float32)
            for k in range(n_tp):
                out = out + (ws[k] * inverse) * orecv[c, k, x, slot].astype(jnp.float32)
            att_ref[c, x, slot] = out.astype(jnp.bfloat16)
            return 0

        lax.fori_loop(0, bq * ns, one, 0)

    for c in range(nc):
        spread(c)
        if c:
            attend(c - 1)
    attend(nc - 1)
    for c in range(nc):
        merge(c)
    for c in range(nc):
        for copy in zsends[c] + xsends[c] + osends[c] + lsends[c]:
            copy.wait_send()


def gather_attend(qm, kv, head_of_slot, lengths, dims):
    nc, bq, nsq, hl, ns, per_tp, Lb, hd, G, T = dims
    n_tp, n_seq = lax.axis_size("tp"), lax.axis_size("seq")
    rows = G * T
    bf, f32 = jnp.bfloat16, jnp.float32
    dma = pltpu.SemaphoreType.DMA
    vmem = pl.BlockSpec(memory_space=pltpu.VMEM)
    smem = pl.BlockSpec(memory_space=pltpu.SMEM)
    return pl.pallas_call(
        functools.partial(gather_attend_kernel, dims),
        out_shape=jax.ShapeDtypeStruct((nc, bq, ns, hd, rows), bf),
        in_specs=[smem, smem, vmem, vmem],
        out_specs=vmem,
        scratch_shapes=[
            [pltpu.VMEM((n_tp, hl, nsq, G, T, hd), bf)] * nc,
            pltpu.VMEM((nc, n_seq, ns, nsq, G, T, hd), bf),
            pltpu.VMEM((nc, n_seq, ns, nsq, G, T, hd), bf),
            pltpu.VMEM((nc, n_tp, bq, ns, hd, rows), bf),
            pltpu.VMEM((nc, n_tp, bq, ns, hd, rows), bf),
            pltpu.VMEM((nc, n_tp, bq, ns, 1, rows), f32),
            pltpu.VMEM((nc, n_tp, bq, ns, 1, rows), f32),
            pltpu.VMEM((Lb, rows), f32),
            dma((nc, n_tp)), dma((nc, n_tp)), dma((nc, n_seq)), dma((nc, n_seq)),
            dma((nc, n_tp)), dma((nc, n_tp)), dma((nc, n_tp)), dma((nc, n_tp)), dma((nc,)),
        ],
        compiler_params=pltpu.CompilerParams(
            collective_id=0, has_side_effects=True, vmem_limit_bytes=56 * 2**20
        ),
    )(head_of_slot, lengths, qm, kv)


def project_kernel(
    dims, soh, att_ref, w_hbm, out_ref,
    w_ref, xr, zs, zr, ag, own, ps, pr,
    x_s, x_r, z_s, z_r, a_s, a_r, p_s, p_r, w_sem, own_sem,
):
    nc, bq, hl, ns, sub, part, T = dims
    n_tp, n_seq = lax.axis_size("tp"), lax.axis_size("seq")
    me_t, me_s = lax.axis_index("tp"), lax.axis_index("seq")
    width, columns = w_ref.shape
    few = bq * sub
    load = pltpu.make_async_copy(w_hbm, w_ref, w_sem)
    greet(("tp", "seq"))
    xsends = [
        [
            remote(att_ref.at[c, lax.rem(me_s + k, n_seq)], xr[c].at[k], x_s.at[c, k], x_r.at[c, k], "seq", k)
            for k in range(1, n_seq)
        ]
        for c in range(nc)
    ]
    owns = [pltpu.make_async_copy(att_ref.at[c, me_s], xr[c].at[0], own_sem.at[c]) for c in range(nc)]
    for c in range(nc):
        for copy in xsends[c]:
            copy.start()
        owns[c].start()
    load.start()
    zsends = [
        [remote(zs.at[c, k], zr.at[c, k], z_s.at[c, k], z_r.at[c, k], "tp", k) for k in range(1, n_tp)]
        for c in range(nc)
    ]
    asends = [
        [remote(zr.at[c], ag.at[c, k], a_s.at[c, k], a_r.at[c, k], "seq", k) for k in range(1, n_seq)]
        for c in range(nc)
    ]
    psends = [
        [remote(ps.at[c, k], pr.at[c, k], p_s.at[c, k], p_r.at[c, k], "tp", k) for k in range(1, n_tp)]
        for c in range(nc)
    ]
    for c in range(nc):
        owns[c].wait()
        for copy in xsends[c]:
            copy.wait_recv()
        for k in list(range(1, n_tp)) + [0]:
            target = zr if k == 0 else zs
            plane = lax.rem(me_t + k, n_tp)
            for j in range(hl):
                slot = soh[plane * hl + j]
                picked = xr[c][back("seq", slot // ns), slot % ns]
                target[c, k, :, j * part : (j + 1) * part] = picked
            if k:
                zsends[c][k - 1].start()
    for c in range(nc):
        for copy in zsends[c]:
            copy.wait_recv()
        for copy in asends[c]:
            copy.start()
    load.wait()
    tile = math.gcd(columns, 512)
    for c in range(nc):
        for copy in asends[c]:
            copy.wait_recv()
        pieces = []
        for k in range(n_tp):
            j = (n_tp - k) % n_tp
            for p in range(n_seq):
                pieces.append(zr[c, j] if p == 0 else ag[c, p, j])
        rows = jnp.concatenate(pieces, axis=0)

        def column_tile(i, _):
            at = pl.ds(pl.multiple_of(i * tile, tile), tile)
            product = jnp.dot(rows, w_ref[:, at], preferred_element_type=jnp.float32)
            span = n_seq * few
            own[c, :, at] = product[:span]
            for k in range(1, n_tp):
                ps[c, k, :, at] = product[k * span : (k + 1) * span].astype(jnp.bfloat16)
            return 0

        lax.fori_loop(0, columns // tile, column_tile, 0)
        for copy in psends[c]:
            copy.start()
    for c in range(nc):
        for copy in psends[c]:
            copy.wait_recv()
        for p in range(n_seq):
            column = lax.rem(me_s + n_seq - p, n_seq)
            for x in range(bq):
                at = p * few + x * sub
                total = own[c, at : at + sub]
                for k in range(1, n_tp):
                    total = total + pr[c, k, at : at + sub].astype(jnp.float32)
                out_ref[c * bq + x, pl.ds(pl.multiple_of(column * sub, sub), sub)] = total.astype(jnp.bfloat16)
    for c in range(nc):
        for copy in xsends[c] + zsends[c] + asends[c] + psends[c]:
            copy.wait_send()


def project(att, weight, slot_of_head, dims):
    nc, bq, hl, ns, sub, part, T = dims
    n_tp, n_seq = lax.axis_size("tp"), lax.axis_size("seq")
    width, columns = weight.shape
    few = bq * sub
    bf, f32 = jnp.bfloat16, jnp.float32
    dma = pltpu.SemaphoreType.DMA
    vmem = pl.BlockSpec(memory_space=pltpu.VMEM)
    return pl.pallas_call(
        functools.partial(project_kernel, dims),
        out_shape=jax.ShapeDtypeStruct((nc * bq, T, columns), bf),
        in_specs=[
            pl.BlockSpec(memory_space=pltpu.SMEM), vmem, pl.BlockSpec(memory_space=pl.ANY)
        ],
        out_specs=vmem,
        scratch_shapes=[
            pltpu.VMEM((width, columns), bf),
            [pltpu.VMEM((n_seq, ns, few, part), bf)] * nc,
            pltpu.VMEM((nc, n_tp, few, width), bf),
            pltpu.VMEM((nc, n_tp, few, width), bf),
            pltpu.VMEM((nc, n_seq, n_tp, few, width), bf),
            pltpu.VMEM((nc, n_seq * few, columns), f32),
            pltpu.VMEM((nc, n_tp, n_seq * few, columns), bf),
            pltpu.VMEM((nc, n_tp, n_seq * few, columns), bf),
            dma((nc, n_seq)), dma((nc, n_seq)), dma((nc, n_tp)), dma((nc, n_tp)),
            dma((nc, n_seq)), dma((nc, n_seq)), dma((nc, n_tp)), dma((nc, n_tp)),
            dma(()), dma((nc,)),
        ],
        compiler_params=pltpu.CompilerParams(
            collective_id=1, has_side_effects=True, vmem_limit_bytes=48 * 2**20
        ),
    )(slot_of_head, att, weight)


def local(query, cache, head_of_slot, lengths, out_weight):
    G = HQ // KVH
    n_seq, n_tp = lax.axis_size("seq"), lax.axis_size("tp")
    me_s = lax.axis_index("seq")
    slot_of_head = slot_table(head_of_slot)
    B, T, width = query.shape
    Lb, ns, hd2 = cache.shape[1:]
    hd = hd2 // 2
    hl = KVH // n_tp
    per_tp = B // n_tp
    nc = math.gcd(CHUNKS, per_tp)
    bq = per_tp // nc
    nsq = n_tp * bq // n_seq
    sub = T // n_seq

    chunked = query.reshape(n_tp, nc, bq, T, width).transpose(1, 0, 2, 3, 4)
    chunked = chunked.reshape(nc, n_seq, nsq, T, width)
    mine = lax.dynamic_index_in_dim(chunked, me_s, 1, False)
    qm = mine.reshape(nc, nsq, T, hl, G, hd).transpose(0, 3, 1, 4, 2, 5)
    kv = cache.transpose(2, 0, 1, 3)
    att = gather_attend(
        qm, kv, head_of_slot, lengths, (nc, bq, nsq, hl, ns, per_tp, Lb, hd, G, T)
    )
    att = att.reshape(nc, bq, ns, hd, G, n_seq, sub).transpose(0, 5, 2, 1, 6, 4, 3)
    att = att.reshape(nc, n_seq, ns, bq * sub, G * hd)
    return project(att, out_weight, slot_of_head, (nc, bq, hl, ns, sub, G * hd, T))


def solution(mesh):
    in_specs = (
        P("grp", None, "tp"),
        P("grp", "tp", "seq", None),
        P("grp"),
        P("grp"),
        P("tp", "seq"),
    )
    out_specs = P(("grp", "tp"), None, "seq")
    return jax.shard_map(local, mesh=mesh, in_specs=in_specs, out_specs=out_specs, check_vma=False)
```

```python
import functools
import math

import jax
import jax.numpy as jnp
from jax import lax
from jax.experimental import pallas as pl
from jax.experimental.pallas import tpu as pltpu
from jax.sharding import PartitionSpec as P

HQ = 64
KVH = 8
CHUNKS = 2
MASKED_SCORE = -1e30
FLOOR = -1e29
MESH = pl.DeviceIdType.MESH


def slot_table(head_of_slot):
    slot_total = head_of_slot.shape[0]
    slot_ids = jnp.arange(slot_total, dtype=jnp.int32)
    return jnp.sum(
        jnp.where(head_of_slot[None, :] == slot_ids[:, None], slot_ids[None, :], 0), axis=1
    )


def greet(axes):
    barrier = pltpu.get_barrier_semaphore()
    total = 0
    for axis in axes:
        n = lax.axis_size(axis)
        me = lax.axis_index(axis)
        for k in range(1, n):
            pl.semaphore_signal(
                barrier, inc=1, device_id={axis: lax.rem(me + k, n)}, device_id_type=MESH
            )
            total += 1
    pl.semaphore_wait(barrier, total)


def remote(src, dst, send_sem, recv_sem, axis, k):
    n = lax.axis_size(axis)
    target = lax.rem(lax.axis_index(axis) + k, n)
    return pltpu.make_async_remote_copy(
        src_ref=src,
        dst_ref=dst,
        send_sem=send_sem,
        recv_sem=recv_sem,
        device_id={axis: target},
        device_id_type=MESH,
    )


def back(axis, index):
    n = lax.axis_size(axis)
    return lax.rem(lax.axis_index(axis) + n - index, n)


def layer_kernel(
    dims, hos, soh, lens, q_ref, kv_ref, w_hbm, out_ref,
    zq, xs, xr, osend, orecv, lsend, lrecv, scores,
    zq_s, zq_r, xq_s, xq_r, o_s, o_r, l_s, l_r, own_sem,
    att, w_ref, xa, zs, zr, ag, own, ps, pr,
    x_s, x_r, z_s, z_r, a_s, a_r, p_s, p_r, w_sem,
):
    nc, bq, nsq, hl, ns, per_tp, Lb, hd, G, T = dims
    width, columns = w_ref.shape
    sub = T // lax.axis_size("seq")
    few = bq * sub
    part = G * hd
    load = pltpu.make_async_copy(w_hbm, w_ref, w_sem)
    n_tp, n_seq = lax.axis_size("tp"), lax.axis_size("seq")
    me_t, me_s = lax.axis_index("tp"), lax.axis_index("seq")
    rows = G * T
    block = math.gcd(Lb, 256)
    scale = math.log2(math.e) / math.sqrt(hd)
    greet(("tp", "seq"))

    zsends = [
        [remote(q_ref.at[c], zq[c].at[k], zq_s.at[c, k], zq_r.at[c, k], "tp", k) for k in range(1, n_tp)]
        for c in range(nc)
    ]
    owns = [pltpu.make_async_copy(q_ref.at[c], zq[c].at[0], own_sem.at[c]) for c in range(nc)]
    for c in range(nc):
        for copy in zsends[c]:
            copy.start()
        owns[c].start()

    xsends = [
        [remote(xs.at[c, k], xr.at[c, k], xq_s.at[c, k], xq_r.at[c, k], "seq", k) for k in range(1, n_seq)]
        for c in range(nc)
    ]

    def spread(c):
        owns[c].wait()
        for copy in zsends[c]:
            copy.wait_recv()
        for k in list(range(1, n_seq)) + [0]:
            target = xr if k == 0 else xs
            column = lax.rem(me_s + k, n_seq)
            for j in range(ns):
                head = hos[column * ns + j]
                target[c, k, j] = zq[c][back("tp", head // hl), head % hl]
            if k:
                xsends[c][k - 1].start()

    osends = [
        [remote(osend.at[c, k], orecv.at[c, k], o_s.at[c, k], o_r.at[c, k], "tp", k) for k in range(1, n_tp)]
        for c in range(nc)
    ]
    lsends = [
        [remote(lsend.at[c, k], lrecv.at[c, k], l_s.at[c, k], l_r.at[c, k], "tp", k) for k in range(1, n_tp)]
        for c in range(nc)
    ]

    def attend_pair(c, k, pair):
        x, slot = pair // ns, pair % ns
        plane = lax.rem(me_t + k, n_tp)
        local_seq = plane * bq + x
        whole_seq = plane * per_tp + c * bq + x
        source = back("seq", local_seq // nsq)
        queries = xr[c, source, slot, local_seq % nsq].reshape(rows, hd)
        visible_end = lens[whole_seq] - me_t * Lb
        limits = visible_end - T + lax.broadcasted_iota(jnp.int32, (1, rows), 1) % T
        top = jnp.full((1, rows), FLOOR, jnp.float32)
        for i in range(Lb // block):
            s = lax.dot_general(
                kv_ref[slot, whole_seq, i * block : (i + 1) * block, :hd],
                queries,
                (((1,), (1,)), ((), ())),
                preferred_element_type=jnp.float32,
            )
            pos = i * block + lax.broadcasted_iota(jnp.int32, (block, 1), 0)
            s = jnp.where(pos <= limits, s * scale, MASKED_SCORE)
            scores[i * block : (i + 1) * block, :] = s
            top = jnp.maximum(top, jnp.max(s, axis=0, keepdims=True))
        total = jnp.zeros((1, rows), jnp.float32)
        out = jnp.zeros((hd, rows), jnp.float32)
        for i in range(Lb // block):
            w = jnp.exp2(scores[i * block : (i + 1) * block, :] - top)
            total = total + jnp.sum(w, axis=0, keepdims=True)
            out = out + lax.dot_general(
                kv_ref[slot, whole_seq, i * block : (i + 1) * block, hd:],
                w.astype(jnp.bfloat16),
                (((0,), (0,)), ((), ())),
                preferred_element_type=jnp.float32,
            )
        total = jnp.maximum(total, 1e-30)
        o_to, l_to = (orecv, lrecv) if k == 0 else (osend, lsend)
        o_to[c, k, x, slot] = (out / total).astype(jnp.bfloat16)
        l_to[c, k, x, slot] = top + jnp.log2(total)

    def attend(c):
        for copy in xsends[c]:
            copy.wait_recv()
        order = sorted(range(1, n_tp), key=lambda k: abs(k - n_tp / 2)) + [0]
        for k in order:
            lax.fori_loop(0, bq * ns, lambda pair, _: (attend_pair(c, k, pair), 0)[1], 0)
            if k:
                osends[c][k - 1].start()
                lsends[c][k - 1].start()

    asends = [
        [remote(zr.at[c], ag.at[c, k], a_s.at[c, k], a_r.at[c, k], "seq", k) for k in range(1, n_seq)]
        for c in range(nc)
    ]
    rsends = [
        [
            remote(att.at[c, lax.rem(me_s + k, n_seq)], xa[c].at[k], x_s.at[c, k], x_r.at[c, k], "seq", k)
            for k in range(1, n_seq)
        ]
        for c in range(nc)
    ]
    psends = [
        [remote(ps.at[c, k], pr.at[c, k], p_s.at[c, k], p_r.at[c, k], "tp", k) for k in range(1, n_tp)]
        for c in range(nc)
    ]
    hsends = [
        [remote(zs.at[c, k], zr.at[c, k], z_s.at[c, k], z_r.at[c, k], "tp", k) for k in range(1, n_tp)]
        for c in range(nc)
    ]
    keeps = [pltpu.make_async_copy(att.at[c, me_s], xa[c].at[0], own_sem.at[nc + c]) for c in range(nc)]

    def merge(c):
        for k in range(n_tp - 1):
            osends[c][k].wait_recv()
            lsends[c][k].wait_recv()
        for pair in range(bq * ns):
            x, slot = pair // ns, pair % ns
            ls = [lrecv[c, k, x, slot] for k in range(n_tp)]
            top = functools.reduce(jnp.maximum, ls)
            ws = [jnp.exp2(l - top) for l in ls]
            inverse = 1.0 / sum(ws)
            out = jnp.zeros((hd, rows), jnp.float32)
            for k in range(n_tp):
                out = out + (ws[k] * inverse) * orecv[c, k, x, slot].astype(jnp.float32)
            out = out.T.astype(jnp.bfloat16)
            for p in range(n_seq):
                for g in range(G):
                    at = g * T + p * sub
                    att[c, p, slot, x * sub : (x + 1) * sub, g * hd : (g + 1) * hd] = out[at : at + sub]
        for copy in rsends[c]:
            copy.start()
        keeps[c].start()

    def to_planes(c):
        keeps[c].wait()
        for copy in rsends[c]:
            copy.wait_recv()
        for k in list(range(1, n_tp)) + [0]:
            target = zr if k == 0 else zs
            plane = lax.rem(me_t + k, n_tp)
            for j in range(hl):
                slot = soh[plane * hl + j]
                picked = xa[c][back("seq", slot // ns), slot % ns]
                target[c, k, :, j * part : (j + 1) * part] = picked
            if k:
                hsends[c][k - 1].start()

    def to_columns(c):
        for copy in hsends[c]:
            copy.wait_recv()
        for copy in asends[c]:
            copy.start()

    tile = math.gcd(columns, 512)
    span = n_seq * few

    def multiply(c):
        for copy in asends[c]:
            copy.wait_recv()
        pieces = []
        for k in range(n_tp):
            j = (n_tp - k) % n_tp
            for p in range(n_seq):
                pieces.append(zr[c, j] if p == 0 else ag[c, p, j])
        left = jnp.concatenate(pieces, axis=0)

        def column_tile(i, _):
            at = pl.ds(pl.multiple_of(i * tile, tile), tile)
            product = jnp.dot(left, w_ref[:, at], preferred_element_type=jnp.float32)
            own[c, :, at] = product[:span]
            for k in range(1, n_tp):
                ps[c, k, :, at] = product[k * span : (k + 1) * span].astype(jnp.bfloat16)
            return 0

        lax.fori_loop(0, columns // tile, column_tile, 0)
        for copy in psends[c]:
            copy.start()

    def finish(c):
        for copy in psends[c]:
            copy.wait_recv()
        for p in range(n_seq):
            column = lax.rem(me_s + n_seq - p, n_seq)
            for x in range(bq):
                at = p * few + x * sub
                total = own[c, at : at + sub]
                for k in range(1, n_tp):
                    total = total + pr[c, k, at : at + sub].astype(jnp.float32)
                out_ref[c * bq + x, pl.ds(pl.multiple_of(column * sub, sub), sub)] = total.astype(jnp.bfloat16)

    load.start()
    for c in range(nc):
        spread(c)
        attend(c)
        if c:
            merge(c - 1)
            to_planes(c - 1)
    load.wait()
    for c in range(nc):
        if c:
            to_columns(c - 1)
        if c == nc - 1:
            merge(c)
            to_planes(c)
        if c:
            multiply(c - 1)
        if c == nc - 1:
            to_columns(c)
            multiply(c)
    for c in range(nc):
        finish(c)
    for c in range(nc):
        for copy in (
            zsends[c] + xsends[c] + osends[c] + lsends[c] + rsends[c] + hsends[c] + asends[c] + psends[c]
        ):
            copy.wait_send()


def layer(qm, kv, weight, head_of_slot, slot_of_head, lengths, dims):
    nc, bq, nsq, hl, ns, per_tp, Lb, hd, G, T = dims
    n_tp, n_seq = lax.axis_size("tp"), lax.axis_size("seq")
    rows = G * T
    width, columns = weight.shape
    sub = T // n_seq
    few = bq * sub
    bf, f32 = jnp.bfloat16, jnp.float32
    dma = pltpu.SemaphoreType.DMA
    vmem = pl.BlockSpec(memory_space=pltpu.VMEM)
    smem = pl.BlockSpec(memory_space=pltpu.SMEM)
    tp_sem, seq_sem = dma((nc, n_tp)), dma((nc, n_seq))
    return pl.pallas_call(
        functools.partial(layer_kernel, dims),
        out_shape=jax.ShapeDtypeStruct((nc * bq, T, columns), bf),
        in_specs=[smem, smem, smem, vmem, vmem, pl.BlockSpec(memory_space=pl.ANY)],
        out_specs=vmem,
        scratch_shapes=[
            [pltpu.VMEM((n_tp, hl, nsq, G, T, hd), bf)] * nc,
            pltpu.VMEM((nc, n_seq, ns, nsq, G, T, hd), bf),
            pltpu.VMEM((nc, n_seq, ns, nsq, G, T, hd), bf),
            pltpu.VMEM((nc, n_tp, bq, ns, hd, rows), bf),
            pltpu.VMEM((nc, n_tp, bq, ns, hd, rows), bf),
            pltpu.VMEM((nc, n_tp, bq, ns, 1, rows), f32),
            pltpu.VMEM((nc, n_tp, bq, ns, 1, rows), f32),
            pltpu.VMEM((Lb, rows), f32),
            tp_sem, tp_sem, seq_sem, seq_sem, tp_sem, tp_sem, tp_sem, tp_sem, dma((2 * nc,)),
            pltpu.VMEM((nc, n_seq, ns, few, G * hd), bf),
            pltpu.VMEM((width, columns), bf),
            [pltpu.VMEM((n_seq, ns, few, G * hd), bf)] * nc,
            pltpu.VMEM((nc, n_tp, few, width), bf),
            pltpu.VMEM((nc, n_tp, few, width), bf),
            pltpu.VMEM((nc, n_seq, n_tp, few, width), bf),
            pltpu.VMEM((nc, n_seq * few, columns), f32),
            pltpu.VMEM((nc, n_tp, n_seq * few, columns), bf),
            pltpu.VMEM((nc, n_tp, n_seq * few, columns), bf),
            seq_sem, seq_sem, tp_sem, tp_sem, seq_sem, seq_sem, tp_sem, tp_sem, dma(()),
        ],
        compiler_params=pltpu.CompilerParams(
            collective_id=0, has_side_effects=True, vmem_limit_bytes=58 * 2**20
        ),
    )(head_of_slot, slot_of_head, lengths, qm, kv, weight)


def local(query, cache, head_of_slot, lengths, out_weight):
    G = HQ // KVH
    n_seq, n_tp = lax.axis_size("seq"), lax.axis_size("tp")
    me_s = lax.axis_index("seq")
    slot_of_head = slot_table(head_of_slot)
    B, T, width = query.shape
    Lb, ns, hd2 = cache.shape[1:]
    hd = hd2 // 2
    hl = KVH // n_tp
    per_tp = B // n_tp
    nc = math.gcd(CHUNKS, per_tp)
    bq = per_tp // nc
    nsq = n_tp * bq // n_seq

    chunked = query.reshape(n_tp, nc, bq, T, width).transpose(1, 0, 2, 3, 4)
    chunked = chunked.reshape(nc, n_seq, nsq, T, width)
    mine = lax.dynamic_index_in_dim(chunked, me_s, 1, False)
    qm = mine.reshape(nc, nsq, T, hl, G, hd).transpose(0, 3, 1, 4, 2, 5)
    kv = cache.transpose(2, 0, 1, 3)
    dims = (nc, bq, nsq, hl, ns, per_tp, Lb, hd, G, T)
    return layer(qm, kv, out_weight, head_of_slot, slot_of_head, lengths, dims)


def solution(mesh):
    in_specs = (
        P("grp", None, "tp"),
        P("grp", "tp", "seq", None),
        P("grp"),
        P("grp"),
        P("tp", "seq"),
    )
    out_specs = P(("grp", "tp"), None, "seq")
    return jax.shard_map(local, mesh=mesh, in_specs=in_specs, out_specs=out_specs, check_vma=False)
```

```python
import functools
import math

import jax
import jax.numpy as jnp
from jax import lax
from jax.experimental import pallas as pl
from jax.experimental.pallas import tpu as pltpu
from jax.sharding import PartitionSpec as P

HQ = 64
KVH = 8
CHUNKS = 2
MASKED_SCORE = -1e30
FLOOR = -1e29
MESH = pl.DeviceIdType.MESH


def slot_table(head_of_slot):
    slot_total = head_of_slot.shape[0]
    slot_ids = jnp.arange(slot_total, dtype=jnp.int32)
    return jnp.sum(
        jnp.where(head_of_slot[None, :] == slot_ids[:, None], slot_ids[None, :], 0), axis=1
    )


def greet(axes):
    barrier = pltpu.get_barrier_semaphore()
    total = 0
    for axis in axes:
        n = lax.axis_size(axis)
        me = lax.axis_index(axis)
        for k in range(1, n):
            pl.semaphore_signal(
                barrier, inc=1, device_id={axis: lax.rem(me + k, n)}, device_id_type=MESH
            )
            total += 1
    pl.semaphore_wait(barrier, total)


def remote(src, dst, send_sem, recv_sem, axis, k):
    n = lax.axis_size(axis)
    target = lax.rem(lax.axis_index(axis) + k, n)
    return pltpu.make_async_remote_copy(
        src_ref=src,
        dst_ref=dst,
        send_sem=send_sem,
        recv_sem=recv_sem,
        device_id={axis: target},
        device_id_type=MESH,
    )


def back(axis, index):
    n = lax.axis_size(axis)
    return lax.rem(lax.axis_index(axis) + n - index, n)


def gather_attend_kernel(
    dims, hos, lens, q_ref, kv_hbm, att_ref,
    raw, kv_ref, kv_sem, zq, xs, xr, osend, orecv, lsend, lrecv, scores,
    zq_s, zq_r, xq_s, xq_r, o_s, o_r, l_s, l_r, own_sem,
):
    nc, bq, nsq, hl, ns, per_tp, Lb, hd, G, T = dims
    n_tp, n_seq = lax.axis_size("tp"), lax.axis_size("seq")
    me_t, me_s = lax.axis_index("tp"), lax.axis_index("seq")
    rows = G * T
    block = math.gcd(Lb, 256)
    scale = math.log2(math.e) / math.sqrt(hd)
    fetch = pltpu.make_async_copy(kv_hbm, raw, kv_sem)
    fetch.start()
    greet(("tp", "seq"))

    zsends = [
        [remote(q_ref.at[c], zq[c].at[k], zq_s.at[c, k], zq_r.at[c, k], "tp", k) for k in range(1, n_tp)]
        for c in range(nc)
    ]
    owns = [pltpu.make_async_copy(q_ref.at[c], zq[c].at[0], own_sem.at[c]) for c in range(nc)]
    for c in range(nc):
        for copy in zsends[c]:
            copy.start()
        owns[c].start()

    xsends = [
        [remote(xs.at[c, k], xr.at[c, k], xq_s.at[c, k], xq_r.at[c, k], "seq", k) for k in range(1, n_seq)]
        for c in range(nc)
    ]

    def spread(c):
        owns[c].wait()
        for copy in zsends[c]:
            copy.wait_recv()
        for k in list(range(1, n_seq)) + [0]:
            target = xr if k == 0 else xs
            column = lax.rem(me_s + k, n_seq)
            for j in range(ns):
                head = hos[column * ns + j]
                target[c, k, j] = zq[c][back("tp", head // hl), head % hl]
            if k:
                xsends[c][k - 1].start()

    osends = [
        [remote(osend.at[c, k], orecv.at[c, k], o_s.at[c, k], o_r.at[c, k], "tp", k) for k in range(1, n_tp)]
        for c in range(nc)
    ]
    lsends = [
        [remote(lsend.at[c, k], lrecv.at[c, k], l_s.at[c, k], l_r.at[c, k], "tp", k) for k in range(1, n_tp)]
        for c in range(nc)
    ]

    def attend_pair(c, k, pair):
        x, slot = pair // ns, pair % ns
        plane = lax.rem(me_t + k, n_tp)
        local_seq = plane * bq + x
        whole_seq = plane * per_tp + c * bq + x
        source = back("seq", local_seq // nsq)
        queries = xr[c, source, slot, local_seq % nsq].reshape(rows, hd)
        visible_end = lens[whole_seq] - me_t * Lb
        limits = visible_end - T + lax.broadcasted_iota(jnp.int32, (1, rows), 1) % T
        top = jnp.full((1, rows), FLOOR, jnp.float32)
        for i in range(Lb // block):
            s = lax.dot_general(
                kv_ref[slot, whole_seq, i * block : (i + 1) * block, :hd],
                queries,
                (((1,), (1,)), ((), ())),
                preferred_element_type=jnp.float32,
            )
            pos = i * block + lax.broadcasted_iota(jnp.int32, (block, 1), 0)
            s = jnp.where(pos <= limits, s * scale, MASKED_SCORE)
            scores[i * block : (i + 1) * block, :] = s
            top = jnp.maximum(top, jnp.max(s, axis=0, keepdims=True))
        total = jnp.zeros((1, rows), jnp.float32)
        out = jnp.zeros((hd, rows), jnp.float32)
        for i in range(Lb // block):
            w = jnp.exp2(scores[i * block : (i + 1) * block, :] - top)
            total = total + jnp.sum(w, axis=0, keepdims=True)
            out = out + lax.dot_general(
                kv_ref[slot, whole_seq, i * block : (i + 1) * block, hd:],
                w.astype(jnp.bfloat16),
                (((0,), (0,)), ((), ())),
                preferred_element_type=jnp.float32,
            )
        total = jnp.maximum(total, 1e-30)
        o_to, l_to = (orecv, lrecv) if k == 0 else (osend, lsend)
        o_to[c, k, x, slot] = (out / total).astype(jnp.bfloat16)
        l_to[c, k, x, slot] = top + jnp.log2(total)

    def attend(c):
        for copy in xsends[c]:
            copy.wait_recv()
        order = sorted(range(1, n_tp), key=lambda k: abs(k - n_tp / 2)) + [0]
        for k in order:
            lax.fori_loop(0, bq * ns, lambda pair, _: (attend_pair(c, k, pair), 0)[1], 0)
            if k:
                osends[c][k - 1].start()
                lsends[c][k - 1].start()

    def merge(c):
        for k in range(n_tp - 1):
            osends[c][k].wait_recv()
            lsends[c][k].wait_recv()

        def one(pair, _):
            x, slot = pair // ns, pair % ns
            ls = [lrecv[c, k, x, slot] for k in range(n_tp)]
            top = functools.reduce(jnp.maximum, ls)
            ws = [jnp.exp2(l - top) for l in ls]
            inverse = 1.0 / sum(ws)
            out = jnp.zeros((hd, rows), jnp.float32)
            for k in range(n_tp):
                out = out + (ws[k] * inverse) * orecv[c, k, x, slot].astype(jnp.float32)
            att_ref[c, x, slot] = out.astype(jnp.bfloat16)
            return 0

        lax.fori_loop(0, bq * ns, one, 0)

    fetch.wait()
    step = math.gcd(Lb, 128)
    turns = Lb // step

    def split(turn, _):
        at = pl.ds(pl.multiple_of(turn % turns * step, step), step)
        for slot in range(ns):
            kv_ref[slot, turn // turns, at, :] = raw[turn // turns, at, slot, :]
        return 0

    lax.fori_loop(0, raw.shape[0] * turns, split, 0)
    for c in range(nc):
        spread(c)
        if c:
            attend(c - 1)
    attend(nc - 1)
    for c in range(nc):
        merge(c)
    for c in range(nc):
        for copy in zsends[c] + xsends[c] + osends[c] + lsends[c]:
            copy.wait_send()


def gather_attend(qm, kv, head_of_slot, lengths, dims):
    nc, bq, nsq, hl, ns, per_tp, Lb, hd, G, T = dims
    n_tp, n_seq = lax.axis_size("tp"), lax.axis_size("seq")
    rows = G * T
    bf, f32 = jnp.bfloat16, jnp.float32
    dma = pltpu.SemaphoreType.DMA
    vmem = pl.BlockSpec(memory_space=pltpu.VMEM)
    smem = pl.BlockSpec(memory_space=pltpu.SMEM)
    return pl.pallas_call(
        functools.partial(gather_attend_kernel, dims),
        out_shape=jax.ShapeDtypeStruct((nc, bq, ns, hd, rows), bf),
        in_specs=[smem, smem, vmem, pl.BlockSpec(memory_space=pl.ANY)],
        out_specs=vmem,
        scratch_shapes=[
            pltpu.VMEM(kv.shape, bf),
            pltpu.VMEM((ns, kv.shape[0], Lb, 2 * hd), bf),
            dma(()),
            [pltpu.VMEM((n_tp, hl, nsq, G, T, hd), bf)] * nc,
            pltpu.VMEM((nc, n_seq, ns, nsq, G, T, hd), bf),
            pltpu.VMEM((nc, n_seq, ns, nsq, G, T, hd), bf),
            pltpu.VMEM((nc, n_tp, bq, ns, hd, rows), bf),
            pltpu.VMEM((nc, n_tp, bq, ns, hd, rows), bf),
            pltpu.VMEM((nc, n_tp, bq, ns, 1, rows), f32),
            pltpu.VMEM((nc, n_tp, bq, ns, 1, rows), f32),
            pltpu.VMEM((Lb, rows), f32),
            dma((nc, n_tp)), dma((nc, n_tp)), dma((nc, n_seq)), dma((nc, n_seq)),
            dma((nc, n_tp)), dma((nc, n_tp)), dma((nc, n_tp)), dma((nc, n_tp)), dma((nc,)),
        ],
        compiler_params=pltpu.CompilerParams(
            collective_id=0, has_side_effects=True, vmem_limit_bytes=56 * 2**20
        ),
    )(head_of_slot, lengths, qm, kv)


def project_kernel(
    dims, soh, att_ref, w_hbm, out_ref,
    w_ref, xr, zs, zr, ag, own, ps, pr,
    x_s, x_r, z_s, z_r, a_s, a_r, p_s, p_r, w_sem, own_sem,
):
    nc, bq, hl, ns, sub, part, T = dims
    n_tp, n_seq = lax.axis_size("tp"), lax.axis_size("seq")
    me_t, me_s = lax.axis_index("tp"), lax.axis_index("seq")
    width, columns = w_ref.shape
    few = bq * sub
    load = pltpu.make_async_copy(w_hbm, w_ref, w_sem)
    greet(("tp", "seq"))
    xsends = [
        [
            remote(att_ref.at[c, lax.rem(me_s + k, n_seq)], xr[c].at[k], x_s.at[c, k], x_r.at[c, k], "seq", k)
            for k in range(1, n_seq)
        ]
        for c in range(nc)
    ]
    owns = [pltpu.make_async_copy(att_ref.at[c, me_s], xr[c].at[0], own_sem.at[c]) for c in range(nc)]
    for c in range(nc):
        for copy in xsends[c]:
            copy.start()
        owns[c].start()
    load.start()
    zsends = [
        [remote(zs.at[c, k], zr.at[c, k], z_s.at[c, k], z_r.at[c, k], "tp", k) for k in range(1, n_tp)]
        for c in range(nc)
    ]
    asends = [
        [remote(zr.at[c], ag.at[c, k], a_s.at[c, k], a_r.at[c, k], "seq", k) for k in range(1, n_seq)]
        for c in range(nc)
    ]
    psends = [
        [remote(ps.at[c, k], pr.at[c, k], p_s.at[c, k], p_r.at[c, k], "tp", k) for k in range(1, n_tp)]
        for c in range(nc)
    ]
    for c in range(nc):
        owns[c].wait()
        for copy in xsends[c]:
            copy.wait_recv()
        for k in list(range(1, n_tp)) + [0]:
            target = zr if k == 0 else zs
            plane = lax.rem(me_t + k, n_tp)
            for j in range(hl):
                slot = soh[plane * hl + j]
                picked = xr[c][back("seq", slot // ns), slot % ns]
                target[c, k, :, j * part : (j + 1) * part] = picked
            if k:
                zsends[c][k - 1].start()
    for c in range(nc):
        for copy in zsends[c]:
            copy.wait_recv()
        for copy in asends[c]:
            copy.start()
    load.wait()
    tile = math.gcd(columns, 512)
    for c in range(nc):
        for copy in asends[c]:
            copy.wait_recv()
        pieces = []
        for k in range(n_tp):
            j = (n_tp - k) % n_tp
            for p in range(n_seq):
                pieces.append(zr[c, j] if p == 0 else ag[c, p, j])
        rows = jnp.concatenate(pieces, axis=0)

        def column_tile(i, _):
            at = pl.ds(pl.multiple_of(i * tile, tile), tile)
            product = jnp.dot(rows, w_ref[:, at], preferred_element_type=jnp.float32)
            span = n_seq * few
            own[c, :, at] = product[:span]
            for k in range(1, n_tp):
                ps[c, k, :, at] = product[k * span : (k + 1) * span].astype(jnp.bfloat16)
            return 0

        lax.fori_loop(0, columns // tile, column_tile, 0)
        for copy in psends[c]:
            copy.start()
    for c in range(nc):
        for copy in psends[c]:
            copy.wait_recv()
        for p in range(n_seq):
            column = lax.rem(me_s + n_seq - p, n_seq)
            for x in range(bq):
                at = p * few + x * sub
                total = own[c, at : at + sub]
                for k in range(1, n_tp):
                    total = total + pr[c, k, at : at + sub].astype(jnp.float32)
                out_ref[c * bq + x, pl.ds(pl.multiple_of(column * sub, sub), sub)] = total.astype(jnp.bfloat16)
    for c in range(nc):
        for copy in xsends[c] + zsends[c] + asends[c] + psends[c]:
            copy.wait_send()


def project(att, weight, slot_of_head, dims):
    nc, bq, hl, ns, sub, part, T = dims
    n_tp, n_seq = lax.axis_size("tp"), lax.axis_size("seq")
    width, columns = weight.shape
    few = bq * sub
    bf, f32 = jnp.bfloat16, jnp.float32
    dma = pltpu.SemaphoreType.DMA
    vmem = pl.BlockSpec(memory_space=pltpu.VMEM)
    return pl.pallas_call(
        functools.partial(project_kernel, dims),
        out_shape=jax.ShapeDtypeStruct((nc * bq, T, columns), bf),
        in_specs=[
            pl.BlockSpec(memory_space=pltpu.SMEM), vmem, pl.BlockSpec(memory_space=pl.ANY)
        ],
        out_specs=vmem,
        scratch_shapes=[
            pltpu.VMEM((width, columns), bf),
            [pltpu.VMEM((n_seq, ns, few, part), bf)] * nc,
            pltpu.VMEM((nc, n_tp, few, width), bf),
            pltpu.VMEM((nc, n_tp, few, width), bf),
            pltpu.VMEM((nc, n_seq, n_tp, few, width), bf),
            pltpu.VMEM((nc, n_seq * few, columns), f32),
            pltpu.VMEM((nc, n_tp, n_seq * few, columns), bf),
            pltpu.VMEM((nc, n_tp, n_seq * few, columns), bf),
            dma((nc, n_seq)), dma((nc, n_seq)), dma((nc, n_tp)), dma((nc, n_tp)),
            dma((nc, n_seq)), dma((nc, n_seq)), dma((nc, n_tp)), dma((nc, n_tp)),
            dma(()), dma((nc,)),
        ],
        compiler_params=pltpu.CompilerParams(
            collective_id=1, has_side_effects=True, vmem_limit_bytes=48 * 2**20
        ),
    )(slot_of_head, att, weight)


def local(query, cache, head_of_slot, lengths, out_weight):
    G = HQ // KVH
    n_seq, n_tp = lax.axis_size("seq"), lax.axis_size("tp")
    me_s = lax.axis_index("seq")
    slot_of_head = slot_table(head_of_slot)
    B, T, width = query.shape
    Lb, ns, hd2 = cache.shape[1:]
    hd = hd2 // 2
    hl = KVH // n_tp
    per_tp = B // n_tp
    nc = math.gcd(CHUNKS, per_tp)
    bq = per_tp // nc
    nsq = n_tp * bq // n_seq
    sub = T // n_seq

    chunked = query.reshape(n_tp, nc, bq, T, width).transpose(1, 0, 2, 3, 4)
    chunked = chunked.reshape(nc, n_seq, nsq, T, width)
    mine = lax.dynamic_index_in_dim(chunked, me_s, 1, False)
    qm = mine.reshape(nc, nsq, T, hl, G, hd).transpose(0, 3, 1, 4, 2, 5)
    kv = cache
    att = gather_attend(
        qm, kv, head_of_slot, lengths, (nc, bq, nsq, hl, ns, per_tp, Lb, hd, G, T)
    )
    att = att.reshape(nc, bq, ns, hd, G, n_seq, sub).transpose(0, 5, 2, 1, 6, 4, 3)
    att = att.reshape(nc, n_seq, ns, bq * sub, G * hd)
    return project(att, out_weight, slot_of_head, (nc, bq, hl, ns, sub, G * hd, T))


def solution(mesh):
    in_specs = (
        P("grp", None, "tp"),
        P("grp", "tp", "seq", None),
        P("grp"),
        P("grp"),
        P("tp", "seq"),
    )
    out_specs = P(("grp", "tp"), None, "seq")
    return jax.shard_map(local, mesh=mesh, in_specs=in_specs, out_specs=out_specs, check_vma=False)
```
